32 devices in a mesh: tm: 8 (over y, x, core), space: 4 (over z).
Axes of the slice: x: 2, y: 2, z: 4, core: 2. Of those that a mesh axis runs over, the one named last changes fastest.
Arguments:
- trajectory: float32 [64, 256, 1024], P('tm', 'space'), may hold values from -1.2 to 1.2
- initial_state: float32 [256, 1024], P('space'), may hold values from -1 to 1
- residual: float32 [64, 256, 1024], P('tm', 'space'), may hold values from -3000 to 3000
- mobility: float32 [256, 1024], P('space'), may hold values from 20 to 200
Outputs:
- update: float32 [64, 256, 1024], P('tm', 'space')
- reduction: float32 [], replicated
The draws below stay inside these ranges and needn't reach their ends.
All inputs are finite; a program needn't handle non-finite values.
Results may differ from the reference program's by a relative error of at most 0.00015.
Values sent between devices are 32-bit elements; how exact they have to be, the bound alone decides.
A program may use at most 64 MiB of HBM per device.

```python
import math
import jax
import jax.numpy as jnp
from jax import lax

NT = 64
NCOL = 1024
SWEEPS = 16
NROWS = 256


def draw_residual(key, part):
    step_pos = jnp.arange(NT).astype(jnp.float32) / (NT - 1)
    row_pos = jnp.arange(NROWS).astype(jnp.float32) / (NROWS - 1)
    envelope = 40.0 * (1.0 + 2.0 * step_pos)[:, None, None] * (1.0 + 2.0 * row_pos)[None, :, None]
    samples = jnp.clip(jax.random.normal(key, (NT, NROWS, NCOL), jnp.float32), -5.0, 5.0)
    return (envelope * samples).astype(jnp.float32)


def block_levels(rng, shape, shards, least, high):
    def one(position, shards_of):
        heights = jax.random.uniform(jax.random.fold_in(jax.random.fold_in(rng, 6), position), (shards_of,), jnp.float32, least / len(shards), high / len(shards))
        return jnp.repeat(jnp.exp(heights), shape[position] // shards_of).reshape((-1,) + (1,) * (len(shape) - position - 1))

    level = one(*shards[0])
    for cut in shards[1:]:
        level = level * one(*cut)
    return level


def setup_inputs(seed: int = 0) -> dict:
    seeds = jax.random.split(jax.random.key(seed), 5)
    return {
        "trajectory": jnp.clip(jax.random.uniform(seeds[0], (NT, NROWS, NCOL), jnp.float32, -1.2, 1.2) * block_levels(seeds[0], (NT, NROWS, NCOL), ((0, 8), (1, 4)), -0.4, 0.0), -1.2, 1.2),
        "initial_state": jnp.clip(jax.random.uniform(seeds[1], (NROWS, NCOL), jnp.float32, -1.0, 1.0) * block_levels(seeds[1], (NROWS, NCOL), ((0, 4),), -0.4, 0.0), -1.0, 1.0),
        "residual": draw_residual(jax.random.fold_in(seeds[4], 71), 0),
        "mobility": jnp.clip(jnp.exp(math.log(200.0) - 2.3025851 * jax.random.uniform(seeds[3], (NROWS, NCOL), jnp.float32) ** block_levels(seeds[3], (NROWS, NCOL), ((0, 4),), -0.2, 0.2)), 20.0, 200.0),
    }


circ_weight = 0.2
time_step = 0.01
damping = 0.8
reaction_scale = 40.0

def time_tables(step_count):
    positions = jnp.arange(step_count).astype(jnp.float32)
    pair_ids = jnp.arange(step_count // 2).astype(jnp.float32)
    phases = 2.0 * jnp.pi * pair_ids / step_count
    angles = phases[:, None] * positions[None, :]
    forward = jnp.stack([jnp.cos(angles), -jnp.sin(angles)], axis=1).reshape(step_count, step_count)
    row_id = jnp.arange(step_count)[:, None]
    forward = jnp.where(row_id == 1, jnp.cos(jnp.pi * positions)[None, :], forward)
    scaling = jnp.where(jnp.arange(step_count) < 2, 1.0, 2.0) / step_count
    inverse = forward.T * scaling[None, :]
    factor = circ_weight ** (1.0 / step_count)
    shift_pair = (1.0 - factor * jnp.cos(phases)) / time_step
    shifts = jnp.stack([shift_pair, shift_pair], axis=1).reshape(step_count)
    shifts = shifts.at[1].set((1.0 + factor) / time_step)
    coupling = factor * jnp.sin(phases) / time_step
    signed = jnp.stack([-coupling, coupling], axis=1).reshape(step_count)
    weights = circ_weight ** (positions / step_count)
    return (forward, inverse, shifts, signed, weights)

def neg_laplace(values):
    neighbours = jnp.roll(values, 1, axis=1) + jnp.roll(values, -1, axis=1)
    neighbours = neighbours + jnp.roll(values, 1, axis=2) + jnp.roll(values, -1, axis=2)
    return 4.0 * values - neighbours

def partner(values):
    extent = values.shape
    return jnp.flip(values.reshape(extent[0] // 2, 2, extent[1], extent[2]), axis=1).reshape(extent)

def relax_pairs(spectrum, shifts, signed, frozen, mobility):
    shift_col = shifts[:, None, None]
    signed_col = signed[:, None, None]
    diagonal = shift_col + (frozen + 4.0 * mobility)[None]
    partner_diag = partner(diagonal)
    denominator = diagonal * partner_diag + signed_col * signed_col

    def one_sweep(sweep_id, values):
        applied = (shift_col + frozen[None]) * values + mobility[None] * neg_laplace(values) + signed_col * partner(values)
        defect = spectrum - applied
        return values + damping * (partner_diag * defect - signed_col * partner(defect)) / denominator
    return lax.fori_loop(0, SWEEPS, one_sweep, jnp.zeros_like(spectrum))

def precondition(values, frozen, mobility, tables):
    forward, inverse, shifts, signed, weights = tables
    weighted = weights[:, None, None] * values
    spectrum = jnp.einsum('mj,jrc->mrc', forward, weighted, precision=lax.Precision.HIGHEST)
    solved = relax_pairs(spectrum, shifts, signed, frozen, mobility)
    restored = jnp.einsum('jm,mrc->jrc', inverse, solved, precision=lax.Precision.HIGHEST)
    return restored / weights[:, None, None]

def jacobian(values, trajectory, mobility):
    earlier = jnp.concatenate([jnp.zeros_like(values[:1]), values[:-1]], axis=0)
    reaction = reaction_scale * (3.0 * trajectory * trajectory - 1.0)
    return (values - earlier) / time_step + mobility[None] * neg_laplace(values) + reaction * values

def reference(trajectory, initial_state, residual, mobility):
    tables = time_tables(NT)
    frozen = reaction_scale * jnp.maximum(3.0 * initial_state * initial_state - 1.0, 0.0)
    norm_value = jnp.sqrt(jnp.sum(residual * residual))
    unit_residual = residual / norm_value
    direction = precondition(unit_residual, frozen, mobility, tables)
    applied = jacobian(direction, trajectory, mobility)
    projection = jnp.sum(unit_residual * applied)
    rest_part = applied - projection * unit_residual
    remainder = jnp.sum(rest_part * rest_part)
    squared_sum = projection * projection + remainder
    update = norm_value * projection / squared_sum * direction
    reduction = jnp.sqrt(remainder / squared_sum)
    return (update, reduction)
```

```python
import functools
import jax
import jax.numpy as jnp
from jax import lax
from jax.experimental import pallas as pl
from jax.experimental.pallas import tpu as pltpu
from jax.sharding import PartitionSpec as P

NT = 64
SWEEPS = 16


circ_weight = 0.2
time_step = 0.01
damping = 0.8
reaction_scale = 40.0


def padded_2(block, sides, width):
    for axis, dim in sides:
        count = lax.axis_size(axis)
        forward = [(i, i + 1) for i in range(count - 1)]
        forward.append((count - 1, 0))
        backward = [(target, source) for source, target in forward]
        low = lax.ppermute(
            lax.slice_in_dim(block, block.shape[dim] - width, None, axis=dim), axis, forward
        )
        high = lax.ppermute(lax.slice_in_dim(block, 0, width, axis=dim), axis, backward)
        block = jnp.concatenate([low, block, high], axis=dim)
    return block


def passed_along(block, axis, distance):
    devices = range(lax.axis_size(axis))
    route = [(i - distance, i) for i in devices if i - distance in devices]
    return lax.ppermute(block, axis, route)


def time_tables(step_count):
    positions = jnp.arange(step_count).astype(jnp.float32)
    pair_ids = jnp.arange(step_count // 2).astype(jnp.float32)
    phases = 2.0 * jnp.pi * pair_ids / step_count
    angles = phases[:, None] * positions[None, :]
    forward = jnp.stack([jnp.cos(angles), -jnp.sin(angles)], axis=1).reshape(step_count, step_count)
    row_id = jnp.arange(step_count)[:, None]
    forward = jnp.where(row_id == 1, jnp.cos(jnp.pi * positions)[None, :], forward)
    scaling = jnp.where(jnp.arange(step_count) < 2, 1.0, 2.0) / step_count
    inverse = forward.T * scaling[None, :]
    factor = circ_weight ** (1.0 / step_count)
    shift_pair = (1.0 - factor * jnp.cos(phases)) / time_step
    shifts = jnp.stack([shift_pair, shift_pair], axis=1).reshape(step_count)
    shifts = shifts.at[1].set((1.0 + factor) / time_step)
    coupling = factor * jnp.sin(phases) / time_step
    signed = jnp.stack([-coupling, coupling], axis=1).reshape(step_count)
    weights = circ_weight ** (positions / step_count)
    return (forward, inverse, shifts, signed, weights)


def neg_laplace(values):
    padded = padded_2(values, (("space", 1),), 1)
    middle = padded[:, 1:-1, :]
    neighbours = padded[:, 2:, :] + padded[:, :-2, :]
    neighbours = neighbours + jnp.roll(middle, 1, axis=2) + jnp.roll(middle, -1, axis=2)
    return 4.0 * values - neighbours


TILE = 8


def relax_kernel(
    count, shift_ref, signed_ref, spec_ref, base_ref, mob_ref, out_ref,
    state, gain, cross, start_val, sent, halo, send_sem, recv_sem,
):
    coefs, rows, cols = spec_ref.shape
    pairs, tiles = coefs // 2, rows // TILE
    keep = 1.0 - damping
    me = lax.axis_index("space")
    prev, after = lax.rem(me + count - 1, count), lax.rem(me + 1, count)

    barrier = pltpu.get_barrier_semaphore()
    for other in (prev, after):
        pl.semaphore_signal(
            barrier, inc=1, device_id={"space": other}, device_id_type=pl.DeviceIdType.MESH
        )
    pl.semaphore_wait(barrier, 2)

    def edge(slot, q, side):
        return pltpu.make_async_remote_copy(
            src_ref=sent.at[slot, q, side],
            dst_ref=halo.at[slot, q, 1 - side],
            send_sem=send_sem.at[slot, q, side],
            recv_sem=recv_sem.at[slot, q, 1 - side],
            device_id={"space": prev if side == 0 else after},
            device_id_type=pl.DeviceIdType.MESH,
        )

    def send(slot, q):
        for side in range(2):
            edge(slot, q, side).start()

    def prepare(q, _):
        sig_e, sig_o = shift_ref[2 * q], shift_ref[2 * q + 1]
        c_e = signed_ref[2 * q]
        for t in [0, tiles - 1] + list(range(1, tiles - 1)):
            span = pl.ds(t * TILE, TILE)
            mob, base = mob_ref[span, :], base_ref[span, :]
            d_e, d_o = sig_e + base, sig_o + base
            scale = damping / (d_e * d_o + c_e * c_e)
            s_e, s_o = spec_ref[2 * q, span, :], spec_ref[2 * q + 1, span, :]
            b_e = scale * (d_o * s_e - c_e * s_o)
            b_o = scale * (d_e * s_o + c_e * s_e)
            scaled = scale * mob
            gain[2 * q, span, :] = scaled * d_o
            gain[2 * q + 1, span, :] = scaled * d_e
            cross[q, span, :] = scaled * c_e
            start_val[2 * q, span, :] = b_e
            start_val[2 * q + 1, span, :] = b_o
            own = pl.ds((t + 1) * TILE, TILE)
            state[0, 2 * q, own, :] = b_e
            state[0, 2 * q + 1, own, :] = b_o
            if t == 0:
                sent[0, q, 0, 0:1, :] = b_e[0:1]
                sent[0, q, 0, 1:2, :] = b_o[0:1]
            if t == tiles - 1:
                sent[0, q, 1, 0:1, :] = b_e[TILE - 1 :]
                sent[0, q, 1, 1:2, :] = b_o[TILE - 1 :]
                send(0, q)
        return 0

    lax.fori_loop(0, pairs, prepare, 0)

    def around(slot, m, t):
        top = (t + 1) * TILE
        mid = state[slot, m, pl.ds(top, TILE), :]
        total = state[slot, m, pl.ds(top - 1, TILE), :] + state[slot, m, pl.ds(top + 1, TILE), :]
        total = total + (pltpu.roll(mid, 1, 1) + pltpu.roll(mid, cols - 1, 1))
        return mid, total

    def sweep(s, _):
        now = lax.rem(s, 2)
        later = 1 - now

        def one_pair(q, _):
            for side in range(2):
                edge(now, q, side).wait()
            for part in range(2):
                state[now, 2 * q + part, pl.ds(TILE - 1, 1), :] = halo[now, q, 0, part : part + 1, :]
                state[now, 2 * q + part, pl.ds(TILE + rows, 1), :] = halo[now, q, 1, part : part + 1, :]
            for t in [0, tiles - 1] + list(range(1, tiles - 1)):
                span = pl.ds(t * TILE, TILE)
                own = pl.ds((t + 1) * TILE, TILE)
                y_e, n_e = around(now, 2 * q, t)
                y_o, n_o = around(now, 2 * q + 1, t)
                c = cross[q, span, :]
                new_e = keep * y_e + start_val[2 * q, span, :] + (gain[2 * q, span, :] * n_e - c * n_o)
                new_o = keep * y_o + start_val[2 * q + 1, span, :] + (gain[2 * q + 1, span, :] * n_o + c * n_e)
                state[later, 2 * q, own, :] = new_e
                state[later, 2 * q + 1, own, :] = new_o
                if t == 0:
                    sent[later, q, 0, 0:1, :] = new_e[0:1]
                    sent[later, q, 0, 1:2, :] = new_o[0:1]
                if t == tiles - 1:
                    sent[later, q, 1, 0:1, :] = new_e[TILE - 1 :]
                    sent[later, q, 1, 1:2, :] = new_o[TILE - 1 :]

                    @pl.when(s < SWEEPS - 2)
                    def _():
                        send(later, q)

            return 0

        return lax.fori_loop(0, pairs, one_pair, 0)

    lax.fori_loop(0, SWEEPS - 1, sweep, 0)
    last = (SWEEPS - 1) % 2

    def store(m, _):
        out_ref[m] = state[last, m, TILE : TILE + rows, :]
        return 0

    lax.fori_loop(0, coefs, store, 0)


def relax_pairs(spectrum, shifts, signed, frozen, mobility):
    coefs, rows, cols = spectrum.shape
    pairs = coefs // 2
    count = lax.axis_size("space")
    vmem = pl.BlockSpec(memory_space=pltpu.VMEM)
    smem = pl.BlockSpec(memory_space=pltpu.SMEM)
    return pl.pallas_call(
        functools.partial(relax_kernel, count),
        out_shape=jax.ShapeDtypeStruct(spectrum.shape, jnp.float32),
        in_specs=[smem, smem, vmem, vmem, vmem],
        out_specs=vmem,
        scratch_shapes=[
            pltpu.VMEM((2, coefs, rows + 2 * TILE, cols), jnp.float32),
            pltpu.VMEM((coefs, rows, cols), jnp.float32),
            pltpu.VMEM((pairs, rows, cols), jnp.float32),
            pltpu.VMEM((coefs, rows, cols), jnp.float32),
            pltpu.VMEM((2, pairs, 2, 2, cols), jnp.float32),
            pltpu.VMEM((2, pairs, 2, 2, cols), jnp.float32),
            pltpu.SemaphoreType.DMA((2, pairs, 2)),
            pltpu.SemaphoreType.DMA((2, pairs, 2)),
        ],
        compiler_params=pltpu.CompilerParams(
            collective_id=0, has_side_effects=True, vmem_limit_bytes=32 * 1024 * 1024
        ),
    )(shifts, signed, spectrum, frozen + 4.0 * mobility, mobility)


def precondition(values, frozen, mobility, tables):
    forward, inverse, shifts, signed, weights = tables
    steps_dev = values.shape[0]
    time_rank = lax.axis_index("tm")
    offset = time_rank * steps_dev
    own_weights = lax.dynamic_slice_in_dim(weights, offset, steps_dev)
    own_shifts = lax.dynamic_slice_in_dim(shifts, offset, steps_dev)
    own_signed = lax.dynamic_slice_in_dim(signed, offset, steps_dev)
    weighted = own_weights[:, None, None] * values
    spectrum = jnp.einsum(
        "mj,jrc->mrc",
        forward,
        lax.all_to_all(weighted, "tm", split_axis=1, concat_axis=0, tiled=True),
        precision=lax.Precision.HIGHEST,
    )
    owned_part = lax.all_to_all(spectrum, "tm", split_axis=0, concat_axis=1, tiled=True)
    solved = relax_pairs(owned_part, own_shifts, own_signed, frozen, mobility)
    in_time = jnp.einsum(
        "jm,mrc->jrc",
        inverse,
        lax.all_to_all(solved, "tm", split_axis=1, concat_axis=0, tiled=True),
        precision=lax.Precision.HIGHEST,
    )
    restored = lax.all_to_all(in_time, "tm", split_axis=0, concat_axis=1, tiled=True)
    return restored / own_weights[:, None, None]


def jacobian(values, trajectory, mobility):
    arriving = passed_along(values[-1:], "tm", 1)
    earlier = jnp.concatenate([arriving, values[:-1]], axis=0)
    reaction = reaction_scale * (3.0 * trajectory * trajectory - 1.0)
    return (values - earlier) / time_step + mobility[None] * neg_laplace(values) + reaction * values


def on_device(trajectory, initial_state, residual, mobility):
    tables = time_tables(NT)
    frozen = reaction_scale * jnp.maximum(3.0 * initial_state * initial_state - 1.0, 0.0)
    direction = precondition(residual, frozen, mobility, tables)
    applied = jacobian(direction, trajectory, mobility)
    norm_square, cross_sum, squared_applied = lax.psum(
        (jnp.sum(residual * residual), jnp.sum(residual * applied), jnp.sum(applied * applied)),
        ("tm", "space"),
    )
    projection = cross_sum / norm_square
    squared_sum = squared_applied / norm_square
    remainder = jnp.maximum(squared_sum - projection * projection, 0.0)
    update = cross_sum / squared_applied * direction
    reduction = jnp.sqrt(remainder / squared_sum)
    return (update, reduction)


def solution(mesh):
    placed = (P("tm", "space", None), P("space", None), P("tm", "space", None), P("space", None))
    return jax.shard_map(
        on_device,
        mesh=mesh,
        in_specs=placed,
        out_specs=(P("tm", "space", None), P()),
        check_vma=False,
    )
```

```python
import functools
import jax
import jax.numpy as jnp
from jax import lax
from jax.experimental import pallas as pl
from jax.experimental.pallas import tpu as pltpu
from jax.sharding import PartitionSpec as P

NT = 64
SWEEPS = 16


circ_weight = 0.2
time_step = 0.01
damping = 0.8
reaction_scale = 40.0


def padded_2(block, sides, width):
    for axis, dim in sides:
        count = lax.axis_size(axis)
        forward = [(i, i + 1) for i in range(count - 1)]
        forward.append((count - 1, 0))
        backward = [(target, source) for source, target in forward]
        low = lax.ppermute(
            lax.slice_in_dim(block, block.shape[dim] - width, None, axis=dim), axis, forward
        )
        high = lax.ppermute(lax.slice_in_dim(block, 0, width, axis=dim), axis, backward)
        block = jnp.concatenate([low, block, high], axis=dim)
    return block


def passed_along(block, axis, distance):
    devices = range(lax.axis_size(axis))
    route = [(i - distance, i) for i in devices if i - distance in devices]
    return lax.ppermute(block, axis, route)


def time_tables(step_count):
    positions = jnp.arange(step_count).astype(jnp.float32)
    pair_ids = jnp.arange(step_count // 2).astype(jnp.float32)
    phases = 2.0 * jnp.pi * pair_ids / step_count
    angles = phases[:, None] * positions[None, :]
    forward = jnp.stack([jnp.cos(angles), -jnp.sin(angles)], axis=1).reshape(step_count, step_count)
    row_id = jnp.arange(step_count)[:, None]
    forward = jnp.where(row_id == 1, jnp.cos(jnp.pi * positions)[None, :], forward)
    scaling = jnp.where(jnp.arange(step_count) < 2, 1.0, 2.0) / step_count
    inverse = forward.T * scaling[None, :]
    factor = circ_weight ** (1.0 / step_count)
    shift_pair = (1.0 - factor * jnp.cos(phases)) / time_step
    shifts = jnp.stack([shift_pair, shift_pair], axis=1).reshape(step_count)
    shifts = shifts.at[1].set((1.0 + factor) / time_step)
    coupling = factor * jnp.sin(phases) / time_step
    signed = jnp.stack([-coupling, coupling], axis=1).reshape(step_count)
    weights = circ_weight ** (positions / step_count)
    return (forward, inverse, shifts, signed, weights)


def neg_laplace(values):
    padded = padded_2(values, (("space", 1),), 1)
    middle = padded[:, 1:-1, :]
    neighbours = padded[:, 2:, :] + padded[:, :-2, :]
    neighbours = neighbours + jnp.roll(middle, 1, axis=2) + jnp.roll(middle, -1, axis=2)
    return 4.0 * values - neighbours


TILE = 8


def relax_kernel(
    count, shift_ref, signed_ref, spec_ref, base_ref, mob_ref, out_ref,
    state, gain, cross, start_val, sent, halo, send_sem, recv_sem,
):
    coefs, rows, cols = spec_ref.shape
    pairs, tiles = coefs // 2, rows // TILE
    keep = 1.0 - damping
    me = lax.axis_index("space")
    prev, after = lax.rem(me + count - 1, count), lax.rem(me + 1, count)

    barrier = pltpu.get_barrier_semaphore()
    for other in (prev, after):
        pl.semaphore_signal(
            barrier, inc=1, device_id={"space": other}, device_id_type=pl.DeviceIdType.MESH
        )
    pl.semaphore_wait(barrier, 2)

    def edge(slot, q, side):
        return pltpu.make_async_remote_copy(
            src_ref=sent.at[slot, q, side],
            dst_ref=halo.at[slot, q, 1 - side],
            send_sem=send_sem.at[slot, q, side],
            recv_sem=recv_sem.at[slot, q, 1 - side],
            device_id={"space": prev if side == 0 else after},
            device_id_type=pl.DeviceIdType.MESH,
        )

    def send(slot, q):
        for side in range(2):
            edge(slot, q, side).start()

    def prepare(q, _):
        sig_e, sig_o = shift_ref[2 * q], shift_ref[2 * q + 1]
        c_e = signed_ref[2 * q]
        for t in [0, tiles - 1] + list(range(1, tiles - 1)):
            span = pl.ds(t * TILE, TILE)
            mob, base = mob_ref[span, :], base_ref[span, :]
            d_e, d_o = sig_e + base, sig_o + base
            scale = damping / (d_e * d_o + c_e * c_e)
            s_e, s_o = spec_ref[2 * q, span, :], spec_ref[2 * q + 1, span, :]
            b_e = scale * (d_o * s_e - c_e * s_o)
            b_o = scale * (d_e * s_o + c_e * s_e)
            scaled = scale * mob
            gain[2 * q, span, :] = scaled * d_o
            gain[2 * q + 1, span, :] = scaled * d_e
            cross[q, span, :] = scaled * c_e
            start_val[2 * q, span, :] = b_e
            start_val[2 * q + 1, span, :] = b_o
            own = pl.ds((t + 1) * TILE, TILE)
            state[0, 2 * q, own, :] = b_e
            state[0, 2 * q + 1, own, :] = b_o
            if t == 0:
                sent[0, q, 0, 0:1, :] = b_e[0:1]
                sent[0, q, 0, 1:2, :] = b_o[0:1]
            if t == tiles - 1:
                sent[0, q, 1, 0:1, :] = b_e[TILE - 1 :]
                sent[0, q, 1, 1:2, :] = b_o[TILE - 1 :]
                send(0, q)
        return 0

    lax.fori_loop(0, pairs, prepare, 0)

    def around(slot, m, t):
        top = (t + 1) * TILE
        mid = state[slot, m, pl.ds(top, TILE), :]
        total = state[slot, m, pl.ds(top - 1, TILE), :] + state[slot, m, pl.ds(top + 1, TILE), :]
        total = total + (pltpu.roll(mid, 1, 1) + pltpu.roll(mid, cols - 1, 1))
        return mid, total

    def sweep(s, _):
        now = lax.rem(s, 2)
        later = 1 - now

        def one_pair(q, _):
            for side in range(2):
                edge(now, q, side).wait()
            for part in range(2):
                state[now, 2 * q + part, pl.ds(TILE - 1, 1), :] = halo[now, q, 0, part : part + 1, :]
                state[now, 2 * q + part, pl.ds(TILE + rows, 1), :] = halo[now, q, 1, part : part + 1, :]
            for t in [0, tiles - 1] + list(range(1, tiles - 1)):
                span = pl.ds(t * TILE, TILE)
                own = pl.ds((t + 1) * TILE, TILE)
                y_e, n_e = around(now, 2 * q, t)
                y_o, n_o = around(now, 2 * q + 1, t)
                c = cross[q, span, :]
                new_e = keep * y_e + start_val[2 * q, span, :] + (gain[2 * q, span, :] * n_e - c * n_o)
                new_o = keep * y_o + start_val[2 * q + 1, span, :] + (gain[2 * q + 1, span, :] * n_o + c * n_e)
                state[later, 2 * q, own, :] = new_e
                state[later, 2 * q + 1, own, :] = new_o
                if t == 0:
                    sent[later, q, 0, 0:1, :] = new_e[0:1]
                    sent[later, q, 0, 1:2, :] = new_o[0:1]
                if t == tiles - 1:
                    sent[later, q, 1, 0:1, :] = new_e[TILE - 1 :]
                    sent[later, q, 1, 1:2, :] = new_o[TILE - 1 :]

                    @pl.when(s < SWEEPS - 2)
                    def _():
                        send(later, q)

            return 0

        return lax.fori_loop(0, pairs, one_pair, 0)

    lax.fori_loop(0, SWEEPS - 1, sweep, 0)
    last = (SWEEPS - 1) % 2

    def store(m, _):
        out_ref[m] = state[last, m, TILE : TILE + rows, :]
        return 0

    lax.fori_loop(0, coefs, store, 0)


def relax_pairs(spectrum, shifts, signed, frozen, mobility):
    coefs, rows, cols = spectrum.shape
    pairs = coefs // 2
    count = lax.axis_size("space")
    vmem = pl.BlockSpec(memory_space=pltpu.VMEM)
    smem = pl.BlockSpec(memory_space=pltpu.SMEM)
    return pl.pallas_call(
        functools.partial(relax_kernel, count),
        out_shape=jax.ShapeDtypeStruct(spectrum.shape, jnp.float32),
        in_specs=[smem, smem, vmem, vmem, vmem],
        out_specs=vmem,
        scratch_shapes=[
            pltpu.VMEM((2, coefs, rows + 2 * TILE, cols), jnp.float32),
            pltpu.VMEM((coefs, rows, cols), jnp.float32),
            pltpu.VMEM((pairs, rows, cols), jnp.float32),
            pltpu.VMEM((coefs, rows, cols), jnp.float32),
            pltpu.VMEM((2, pairs, 2, 2, cols), jnp.float32),
            pltpu.VMEM((2, pairs, 2, 2, cols), jnp.float32),
            pltpu.SemaphoreType.DMA((2, pairs, 2)),
            pltpu.SemaphoreType.DMA((2, pairs, 2)),
        ],
        compiler_params=pltpu.CompilerParams(
            collective_id=0, has_side_effects=True, vmem_limit_bytes=32 * 1024 * 1024
        ),
    )(shifts, signed, spectrum, frozen + 4.0 * mobility, mobility)


def precondition(values, frozen, mobility, tables):
    forward, inverse, shifts, signed, weights = tables
    steps_dev = values.shape[0]
    time_rank = lax.axis_index("tm")
    offset = time_rank * steps_dev
    own_weights = lax.dynamic_slice_in_dim(weights, offset, steps_dev)
    own_shifts = lax.dynamic_slice_in_dim(shifts, offset, steps_dev)
    own_signed = lax.dynamic_slice_in_dim(signed, offset, steps_dev)
    weighted = own_weights[:, None, None] * values
    spectrum = jnp.einsum(
        "mj,jrc->mrc",
        forward,
        lax.all_to_all(weighted, "tm", split_axis=1, concat_axis=0, tiled=True),
        precision=lax.Precision.HIGHEST,
    )
    owned_part = lax.all_to_all(spectrum, "tm", split_axis=0, concat_axis=1, tiled=True)
    solved = relax_pairs(owned_part, own_shifts, own_signed, frozen, mobility)
    in_time = jnp.einsum(
        "jm,mrc->jrc",
        inverse,
        lax.all_to_all(solved, "tm", split_axis=1, concat_axis=0, tiled=True),
        precision=lax.Precision.HIGHEST,
    )
    restored = lax.all_to_all(in_time, "tm", split_axis=0, concat_axis=1, tiled=True)
    return restored / own_weights[:, None, None]


LANES = 128


def block_kernel(
    z_count, t_count, shift_ref, signed_ref, spec_ref, base_ref, mob_ref, out_ref,
    state, gain, cross, start_val, z_sent, z_halo, c_sent, c_halo,
    z_send, z_recv, c_send, c_recv,
):
    coefs, rows, cols = spec_ref.shape
    tiles = rows // TILE
    per = LANES // tiles
    groups = coefs // per
    keep = 1.0 - damping
    z_me, t_me = lax.axis_index("space"), lax.axis_index("tm")
    z_to = (lax.rem(z_me + z_count - 1, z_count), lax.rem(z_me + 1, z_count))
    t_to = (lax.rem(t_me + t_count - 1, t_count), lax.rem(t_me + 1, t_count))
    lane = lax.broadcasted_iota(jnp.int32, (TILE, LANES), 1)
    order = [0, tiles - 1] + list(range(1, tiles - 1))

    barrier = pltpu.get_barrier_semaphore()
    for axis, others in (("space", z_to), ("tm", t_to)):
        for other in others:
            pl.semaphore_signal(
                barrier, inc=1, device_id={axis: other}, device_id_type=pl.DeviceIdType.MESH
            )
    pl.semaphore_wait(barrier, 4)

    def copies(slot, g):
        made = []
        for axis, to, src, dst, snd, rcv in (
            ("space", z_to, z_sent, z_halo, z_send, z_recv),
            ("tm", t_to, c_sent, c_halo, c_send, c_recv),
        ):
            for side in range(2):
                made.append(
                    pltpu.make_async_remote_copy(
                        src_ref=src.at[slot, g, side],
                        dst_ref=dst.at[slot, g, 1 - side],
                        send_sem=snd.at[slot, g, side],
                        recv_sem=rcv.at[slot, g, 1 - side],
                        device_id={axis: to[side]},
                        device_id_type=pl.DeviceIdType.MESH,
                    )
                )
        return made

    def keep_edges(slot, g, i, t, value, low, high):
        if t == 0:
            z_sent[slot, g, 0, i : i + 1, :] = value[0:1]
        if t == tiles - 1:
            z_sent[slot, g, 1, i : i + 1, :] = value[TILE - 1 :]
        k = t * per + i
        turned = pltpu.roll(value, k, 1) if k else value
        low = jnp.where(lane == k, turned, low)
        high = jnp.where(lane == (k - 1) % LANES, turned, high)
        return low, high

    def prepare(g, _):
        low = high = jnp.zeros((TILE, LANES), jnp.float32)
        for p in range(per // 2):
            q = g * (per // 2) + p
            sig_e, sig_o = shift_ref[2 * q], shift_ref[2 * q + 1]
            c_e = signed_ref[2 * q]
            for t in order:
                span = pl.ds(t * TILE, TILE)
                mob, base = mob_ref[span, :], base_ref[span, :]
                d_e, d_o = sig_e + base, sig_o + base
                scale = damping / (d_e * d_o + c_e * c_e)
                s_e, s_o = spec_ref[2 * q, span, :], spec_ref[2 * q + 1, span, :]
                b_e = scale * (d_o * s_e - c_e * s_o)
                b_o = scale * (d_e * s_o + c_e * s_e)
                scaled = scale * mob
                gain[2 * q, span, :] = scaled * d_o
                gain[2 * q + 1, span, :] = scaled * d_e
                cross[q, span, :] = scaled * c_e
                start_val[2 * q, span, :] = b_e
                start_val[2 * q + 1, span, :] = b_o
                own = pl.ds((t + 1) * TILE, TILE)
                state[0, 2 * q, own, :] = b_e
                state[0, 2 * q + 1, own, :] = b_o
                low, high = keep_edges(0, g, 2 * p, t, b_e, low, high)
                low, high = keep_edges(0, g, 2 * p + 1, t, b_o, low, high)
        c_sent[0, g, 0] = low
        c_sent[0, g, 1] = high
        for copy in copies(0, g):
            copy.start()
        return 0

    lax.fori_loop(0, groups, prepare, 0)

    def sweep(s, _):
        now = lax.rem(s, 2)
        later = 1 - now

        def one_group(g, _):
            for copy in copies(now, g):
                copy.wait()
            from_left, from_right = c_halo[now, g, 0], c_halo[now, g, 1]
            low = high = jnp.zeros((TILE, LANES), jnp.float32)

            def around(m, i, t):
                top = (t + 1) * TILE
                mid = state[now, m, pl.ds(top, TILE), :]
                k = t * per + i
                edge = jnp.where(lane == k, from_right, from_left)
                edge = pltpu.roll(edge, LANES - k, 1) if k else edge
                total = state[now, m, pl.ds(top - 1, TILE), :] + state[now, m, pl.ds(top + 1, TILE), :]
                right = pltpu.roll(jnp.where(lane == 0, edge, mid), LANES - 1, 1)
                left = pltpu.roll(jnp.where(lane == LANES - 1, edge, mid), 1, 1)
                return mid, total + (left + right)

            for p in range(per // 2):
                q = g * (per // 2) + p
                for part in range(2):
                    i = 2 * p + part
                    state[now, 2 * q + part, pl.ds(TILE - 1, 1), :] = z_halo[now, g, 0, i : i + 1, :]
                    state[now, 2 * q + part, pl.ds(TILE + rows, 1), :] = z_halo[now, g, 1, i : i + 1, :]
                for t in order:
                    span = pl.ds(t * TILE, TILE)
                    own = pl.ds((t + 1) * TILE, TILE)
                    y_e, n_e = around(2 * q, 2 * p, t)
                    y_o, n_o = around(2 * q + 1, 2 * p + 1, t)
                    c = cross[q, span, :]
                    new_e = keep * y_e + start_val[2 * q, span, :] + (gain[2 * q, span, :] * n_e - c * n_o)
                    new_o = keep * y_o + start_val[2 * q + 1, span, :] + (gain[2 * q + 1, span, :] * n_o + c * n_e)
                    state[later, 2 * q, own, :] = new_e
                    state[later, 2 * q + 1, own, :] = new_o
                    low, high = keep_edges(later, g, 2 * p, t, new_e, low, high)
                    low, high = keep_edges(later, g, 2 * p + 1, t, new_o, low, high)
            c_sent[later, g, 0] = low
            c_sent[later, g, 1] = high

            @pl.when(s < SWEEPS - 2)
            def _():
                for copy in copies(later, g):
                    copy.start()

            return 0

        return lax.fori_loop(0, groups, one_group, 0)

    lax.fori_loop(0, SWEEPS - 1, sweep, 0)
    last = (SWEEPS - 1) % 2

    def store(m, _):
        out_ref[m] = state[last, m, TILE : TILE + rows, :]
        return 0

    lax.fori_loop(0, coefs, store, 0)


def fits_block(coefs, rows, cols):
    tiles = rows // TILE
    return (
        cols == LANES and rows % TILE == 0 and LANES % tiles == 0
        and (LANES // tiles) % 8 == 0 and coefs % (LANES // tiles) == 0
    )


def relax_block(spectrum, shifts, signed, frozen, mobility):
    coefs, rows, cols = spectrum.shape
    per = LANES // (rows // TILE)
    groups = coefs // per
    vmem = pl.BlockSpec(memory_space=pltpu.VMEM)
    smem = pl.BlockSpec(memory_space=pltpu.SMEM)
    sems = pltpu.SemaphoreType.DMA((2, groups, 2))
    return pl.pallas_call(
        functools.partial(block_kernel, lax.axis_size("space"), lax.axis_size("tm")),
        out_shape=jax.ShapeDtypeStruct(spectrum.shape, jnp.float32),
        in_specs=[smem, smem, vmem, vmem, vmem],
        out_specs=vmem,
        scratch_shapes=[
            pltpu.VMEM((2, coefs, rows + 2 * TILE, cols), jnp.float32),
            pltpu.VMEM((coefs, rows, cols), jnp.float32),
            pltpu.VMEM((coefs // 2, rows, cols), jnp.float32),
            pltpu.VMEM((coefs, rows, cols), jnp.float32),
            pltpu.VMEM((2, groups, 2, per, cols), jnp.float32),
            pltpu.VMEM((2, groups, 2, per, cols), jnp.float32),
            pltpu.VMEM((2, groups, 2, TILE, LANES), jnp.float32),
            pltpu.VMEM((2, groups, 2, TILE, LANES), jnp.float32),
            sems, sems, sems, sems,
        ],
        compiler_params=pltpu.CompilerParams(
            collective_id=1, has_side_effects=True, vmem_limit_bytes=32 * 1024 * 1024
        ),
    )(shifts, signed, spectrum, frozen + 4.0 * mobility, mobility)


def precondition_columns(values, frozen, mobility, tables):
    forward, inverse, shifts, signed, weights = tables
    width = values.shape[2] // lax.axis_size("tm")
    first = lax.axis_index("tm") * width
    own_frozen = lax.dynamic_slice_in_dim(frozen, first, width, axis=1)
    own_mobility = lax.dynamic_slice_in_dim(mobility, first, width, axis=1)
    weighted = forward * weights[None, :]
    gathered = lax.all_to_all(values, "tm", split_axis=2, concat_axis=0, tiled=True)
    spectrum = jnp.einsum("mj,jrc->mrc", weighted, gathered, precision=lax.Precision.HIGHEST)
    solved = relax_block(spectrum, shifts, signed, own_frozen, own_mobility)
    restoring = inverse / weights[:, None]
    in_time = jnp.einsum("jm,mrc->jrc", restoring, solved, precision=lax.Precision.HIGHEST)
    return lax.all_to_all(in_time, "tm", split_axis=0, concat_axis=2, tiled=True)


def sum_kernel(t_count, z_count, x_ref, out_ref, t_got, z_own, z_got, t_send, t_recv, z_send, z_recv):
    barrier = pltpu.get_barrier_semaphore()
    places = (("tm", t_count), ("space", z_count))
    for axis, count in places:
        me = lax.axis_index(axis)
        for k in range(1, count):
            pl.semaphore_signal(
                barrier, inc=1, device_id={axis: lax.rem(me + k, count)},
                device_id_type=pl.DeviceIdType.MESH,
            )
    pl.semaphore_wait(barrier, t_count + z_count - 2)
    for axis, count, src, got, snd, rcv in (
        ("tm", t_count, x_ref, t_got, t_send, t_recv),
        ("space", z_count, z_own, z_got, z_send, z_recv),
    ):
        me = lax.axis_index(axis)
        made = []
        for k in range(1, count):
            made.append(
                pltpu.make_async_remote_copy(
                    src_ref=src, dst_ref=got.at[me], send_sem=snd.at[k], recv_sem=rcv.at[k],
                    device_id={axis: lax.rem(me + k, count)},
                    device_id_type=pl.DeviceIdType.MESH,
                )
            )
        for copy in made:
            copy.start()
        got[me] = src[...]
        for copy in made:
            copy.wait()
        total = got[0]
        for k in range(1, count):
            total = total + got[k]
        if axis == "tm":
            z_own[...] = total
        else:
            out_ref[...] = total


def summed(parts):
    t_count, z_count = lax.axis_size("tm"), lax.axis_size("space")
    row = lax.broadcasted_iota(jnp.int32, (TILE, LANES), 0)
    packed = jnp.zeros((TILE, LANES), jnp.float32)
    for k, part in enumerate(parts):
        packed = jnp.where(row == k, part, packed)
    vmem = pl.BlockSpec(memory_space=pltpu.VMEM)
    dma = pltpu.SemaphoreType.DMA
    total = pl.pallas_call(
        functools.partial(sum_kernel, t_count, z_count),
        out_shape=jax.ShapeDtypeStruct((TILE, LANES), jnp.float32),
        in_specs=[vmem],
        out_specs=vmem,
        scratch_shapes=[
            pltpu.VMEM((t_count, TILE, LANES), jnp.float32),
            pltpu.VMEM((TILE, LANES), jnp.float32),
            pltpu.VMEM((z_count, TILE, LANES), jnp.float32),
            dma((t_count,)), dma((t_count,)), dma((z_count,)), dma((z_count,)),
        ],
        compiler_params=pltpu.CompilerParams(
            collective_id=2, has_side_effects=True, vmem_limit_bytes=4 * 1024 * 1024
        ),
    )(packed)
    return [total[k, 0] for k in range(len(parts))]


def jacobian(values, trajectory, mobility):
    arriving = passed_along(values[-1:], "tm", 1)
    earlier = jnp.concatenate([arriving, values[:-1]], axis=0)
    reaction = reaction_scale * (3.0 * trajectory * trajectory - 1.0)
    return (values - earlier) / time_step + mobility[None] * neg_laplace(values) + reaction * values


def on_device(trajectory, initial_state, residual, mobility):
    tables = time_tables(NT)
    frozen = reaction_scale * jnp.maximum(3.0 * initial_state * initial_state - 1.0, 0.0)
    steps_dev, rows, cols = residual.shape
    shards = lax.axis_size("tm")
    by_columns = cols % shards == 0 and fits_block(NT, rows, cols // shards)
    run = precondition_columns if by_columns else precondition
    direction = run(residual, frozen, mobility, tables)
    applied = jacobian(direction, trajectory, mobility)
    norm_square, cross_sum, squared_applied = summed(
        (jnp.sum(residual * residual), jnp.sum(residual * applied), jnp.sum(applied * applied))
    )
    projection = cross_sum / norm_square
    squared_sum = squared_applied / norm_square
    remainder = jnp.maximum(squared_sum - projection * projection, 0.0)
    update = cross_sum / squared_applied * direction
    reduction = jnp.sqrt(remainder / squared_sum)
    return (update, reduction)


def solution(mesh):
    placed = (P("tm", "space", None), P("space", None), P("tm", "space", None), P("space", None))
    return jax.shard_map(
        on_device,
        mesh=mesh,
        in_specs=placed,
        out_specs=(P("tm", "space", None), P()),
        check_vma=False,
    )
```

```python
import functools
import jax
import jax.numpy as jnp
from jax import lax
from jax.experimental import pallas as pl
from jax.experimental.pallas import tpu as pltpu
from jax.sharding import PartitionSpec as P

NT = 64
SWEEPS = 16


circ_weight = 0.2
time_step = 0.01
damping = 0.8
reaction_scale = 40.0


def padded_2(block, sides, width):
    for axis, dim in sides:
        count = lax.axis_size(axis)
        forward = [(i, i + 1) for i in range(count - 1)]
        forward.append((count - 1, 0))
        backward = [(target, source) for source, target in forward]
        low = lax.ppermute(
            lax.slice_in_dim(block, block.shape[dim] - width, None, axis=dim), axis, forward
        )
        high = lax.ppermute(lax.slice_in_dim(block, 0, width, axis=dim), axis, backward)
        block = jnp.concatenate([low, block, high], axis=dim)
    return block


def passed_along(block, axis, distance):
    devices = range(lax.axis_size(axis))
    route = [(i - distance, i) for i in devices if i - distance in devices]
    return lax.ppermute(block, axis, route)


def time_tables(step_count):
    positions = jnp.arange(step_count).astype(jnp.float32)
    pair_ids = jnp.arange(step_count // 2).astype(jnp.float32)
    phases = 2.0 * jnp.pi * pair_ids / step_count
    angles = phases[:, None] * positions[None, :]
    forward = jnp.stack([jnp.cos(angles), -jnp.sin(angles)], axis=1).reshape(step_count, step_count)
    row_id = jnp.arange(step_count)[:, None]
    forward = jnp.where(row_id == 1, jnp.cos(jnp.pi * positions)[None, :], forward)
    scaling = jnp.where(jnp.arange(step_count) < 2, 1.0, 2.0) / step_count
    inverse = forward.T * scaling[None, :]
    factor = circ_weight ** (1.0 / step_count)
    shift_pair = (1.0 - factor * jnp.cos(phases)) / time_step
    shifts = jnp.stack([shift_pair, shift_pair], axis=1).reshape(step_count)
    shifts = shifts.at[1].set((1.0 + factor) / time_step)
    coupling = factor * jnp.sin(phases) / time_step
    signed = jnp.stack([-coupling, coupling], axis=1).reshape(step_count)
    weights = circ_weight ** (positions / step_count)
    return (forward, inverse, shifts, signed, weights)


def neg_laplace(values):
    padded = padded_2(values, (("space", 1),), 1)
    middle = padded[:, 1:-1, :]
    neighbours = padded[:, 2:, :] + padded[:, :-2, :]
    neighbours = neighbours + jnp.roll(middle, 1, axis=2) + jnp.roll(middle, -1, axis=2)
    return 4.0 * values - neighbours


TILE = 8


def relax_kernel(
    count, shift_ref, signed_ref, spec_ref, base_ref, mob_ref, out_ref,
    state, gain, cross, start_val, sent, halo, send_sem, recv_sem,
):
    coefs, rows, cols = spec_ref.shape
    pairs, tiles = coefs // 2, rows // TILE
    keep = 1.0 - damping
    me = lax.axis_index("space")
    prev, after = lax.rem(me + count - 1, count), lax.rem(me + 1, count)

    barrier = pltpu.get_barrier_semaphore()
    for other in (prev, after):
        pl.semaphore_signal(
            barrier, inc=1, device_id={"space": other}, device_id_type=pl.DeviceIdType.MESH
        )
    pl.semaphore_wait(barrier, 2)

    def edge(slot, q, side):
        return pltpu.make_async_remote_copy(
            src_ref=sent.at[slot, q, side],
            dst_ref=halo.at[slot, q, 1 - side],
            send_sem=send_sem.at[slot, q, side],
            recv_sem=recv_sem.at[slot, q, 1 - side],
            device_id={"space": prev if side == 0 else after},
            device_id_type=pl.DeviceIdType.MESH,
        )

    def send(slot, q):
        for side in range(2):
            edge(slot, q, side).start()

    def prepare(q, _):
        sig_e, sig_o = shift_ref[2 * q], shift_ref[2 * q + 1]
        c_e = signed_ref[2 * q]
        for t in [0, tiles - 1] + list(range(1, tiles - 1)):
            span = pl.ds(t * TILE, TILE)
            mob, base = mob_ref[span, :], base_ref[span, :]
            d_e, d_o = sig_e + base, sig_o + base
            scale = damping / (d_e * d_o + c_e * c_e)
            s_e, s_o = spec_ref[2 * q, span, :], spec_ref[2 * q + 1, span, :]
            b_e = scale * (d_o * s_e - c_e * s_o)
            b_o = scale * (d_e * s_o + c_e * s_e)
            scaled = scale * mob
            gain[2 * q, span, :] = scaled * d_o
            gain[2 * q + 1, span, :] = scaled * d_e
            cross[q, span, :] = scaled * c_e
            start_val[2 * q, span, :] = b_e
            start_val[2 * q + 1, span, :] = b_o
            own = pl.ds((t + 1) * TILE, TILE)
            state[0, 2 * q, own, :] = b_e
            state[0, 2 * q + 1, own, :] = b_o
            if t == 0:
                sent[0, q, 0, 0:1, :] = b_e[0:1]
                sent[0, q, 0, 1:2, :] = b_o[0:1]
            if t == tiles - 1:
                sent[0, q, 1, 0:1, :] = b_e[TILE - 1 :]
                sent[0, q, 1, 1:2, :] = b_o[TILE - 1 :]
                send(0, q)
        return 0

    lax.fori_loop(0, pairs, prepare, 0)

    def around(slot, m, t):
        top = (t + 1) * TILE
        mid = state[slot, m, pl.ds(top, TILE), :]
        total = state[slot, m, pl.ds(top - 1, TILE), :] + state[slot, m, pl.ds(top + 1, TILE), :]
        total = total + (pltpu.roll(mid, 1, 1) + pltpu.roll(mid, cols - 1, 1))
        return mid, total

    def sweep(s, _):
        now = lax.rem(s, 2)
        later = 1 - now

        def one_pair(q, _):
            for side in range(2):
                edge(now, q, side).wait()
            for part in range(2):
                state[now, 2 * q + part, pl.ds(TILE - 1, 1), :] = halo[now, q, 0, part : part + 1, :]
                state[now, 2 * q + part, pl.ds(TILE + rows, 1), :] = halo[now, q, 1, part : part + 1, :]
            for t in [0, tiles - 1] + list(range(1, tiles - 1)):
                span = pl.ds(t * TILE, TILE)
                own = pl.ds((t + 1) * TILE, TILE)
                y_e, n_e = around(now, 2 * q, t)
                y_o, n_o = around(now, 2 * q + 1, t)
                c = cross[q, span, :]
                new_e = keep * y_e + start_val[2 * q, span, :] + (gain[2 * q, span, :] * n_e - c * n_o)
                new_o = keep * y_o + start_val[2 * q + 1, span, :] + (gain[2 * q + 1, span, :] * n_o + c * n_e)
                state[later, 2 * q, own, :] = new_e
                state[later, 2 * q + 1, own, :] = new_o
                if t == 0:
                    sent[later, q, 0, 0:1, :] = new_e[0:1]
                    sent[later, q, 0, 1:2, :] = new_o[0:1]
                if t == tiles - 1:
                    sent[later, q, 1, 0:1, :] = new_e[TILE - 1 :]
                    sent[later, q, 1, 1:2, :] = new_o[TILE - 1 :]

                    @pl.when(s < SWEEPS - 2)
                    def _():
                        send(later, q)

            return 0

        return lax.fori_loop(0, pairs, one_pair, 0)

    lax.fori_loop(0, SWEEPS - 1, sweep, 0)
    last = (SWEEPS - 1) % 2

    def store(m, _):
        out_ref[m] = state[last, m, TILE : TILE + rows, :]
        return 0

    lax.fori_loop(0, coefs, store, 0)


def relax_pairs(spectrum, shifts, signed, frozen, mobility):
    coefs, rows, cols = spectrum.shape
    pairs = coefs // 2
    count = lax.axis_size("space")
    vmem = pl.BlockSpec(memory_space=pltpu.VMEM)
    smem = pl.BlockSpec(memory_space=pltpu.SMEM)
    return pl.pallas_call(
        functools.partial(relax_kernel, count),
        out_shape=jax.ShapeDtypeStruct(spectrum.shape, jnp.float32),
        in_specs=[smem, smem, vmem, vmem, vmem],
        out_specs=vmem,
        scratch_shapes=[
            pltpu.VMEM((2, coefs, rows + 2 * TILE, cols), jnp.float32),
            pltpu.VMEM((coefs, rows, cols), jnp.float32),
            pltpu.VMEM((pairs, rows, cols), jnp.float32),
            pltpu.VMEM((coefs, rows, cols), jnp.float32),
            pltpu.VMEM((2, pairs, 2, 2, cols), jnp.float32),
            pltpu.VMEM((2, pairs, 2, 2, cols), jnp.float32),
            pltpu.SemaphoreType.DMA((2, pairs, 2)),
            pltpu.SemaphoreType.DMA((2, pairs, 2)),
        ],
        compiler_params=pltpu.CompilerParams(
            collective_id=0, has_side_effects=True, vmem_limit_bytes=32 * 1024 * 1024
        ),
    )(shifts, signed, spectrum, frozen + 4.0 * mobility, mobility)


def precondition(values, frozen, mobility, tables):
    forward, inverse, shifts, signed, weights = tables
    steps_dev = values.shape[0]
    time_rank = lax.axis_index("tm")
    offset = time_rank * steps_dev
    own_weights = lax.dynamic_slice_in_dim(weights, offset, steps_dev)
    own_shifts = lax.dynamic_slice_in_dim(shifts, offset, steps_dev)
    own_signed = lax.dynamic_slice_in_dim(signed, offset, steps_dev)
    weighted = own_weights[:, None, None] * values
    spectrum = jnp.einsum(
        "mj,jrc->mrc",
        forward,
        lax.all_to_all(weighted, "tm", split_axis=1, concat_axis=0, tiled=True),
        precision=lax.Precision.HIGHEST,
    )
    owned_part = lax.all_to_all(spectrum, "tm", split_axis=0, concat_axis=1, tiled=True)
    solved = relax_pairs(owned_part, own_shifts, own_signed, frozen, mobility)
    in_time = jnp.einsum(
        "jm,mrc->jrc",
        inverse,
        lax.all_to_all(solved, "tm", split_axis=1, concat_axis=0, tiled=True),
        precision=lax.Precision.HIGHEST,
    )
    restored = lax.all_to_all(in_time, "tm", split_axis=0, concat_axis=1, tiled=True)
    return restored / own_weights[:, None, None]


LANES = 128


def block_kernel(
    z_count, t_count, shift_ref, signed_ref, spec_ref, base_ref, mob_ref, out_ref,
    state_a, state_b, gain, cross, start_val, z_sent, z_halo, c_sent, c_halo,
    z_send, z_recv, c_send, c_recv,
):
    coefs, rows, cols = spec_ref.shape
    tiles = rows // TILE
    per = LANES // tiles
    groups = coefs // per
    keep = 1.0 - damping
    z_me, t_me = lax.axis_index("space"), lax.axis_index("tm")
    z_to = (lax.rem(z_me + z_count - 1, z_count), lax.rem(z_me + 1, z_count))
    t_to = (lax.rem(t_me + t_count - 1, t_count), lax.rem(t_me + 1, t_count))
    lane = lax.broadcasted_iota(jnp.int32, (TILE, LANES), 1)
    order = [0, tiles - 1] + list(range(1, tiles - 1))

    barrier = pltpu.get_barrier_semaphore()
    for axis, others in (("space", z_to), ("tm", t_to)):
        for other in others:
            pl.semaphore_signal(
                barrier, inc=1, device_id={axis: other}, device_id_type=pl.DeviceIdType.MESH
            )
    pl.semaphore_wait(barrier, 4)

    def copies(slot, g):
        made = []
        for axis, to, src, dst, snd, rcv in (
            ("space", z_to, z_sent, z_halo, z_send, z_recv),
            ("tm", t_to, c_sent, c_halo, c_send, c_recv),
        ):
            for side in range(2):
                made.append(
                    pltpu.make_async_remote_copy(
                        src_ref=src.at[slot, g, side],
                        dst_ref=dst.at[slot, g, 1 - side],
                        send_sem=snd.at[slot, g, side],
                        recv_sem=rcv.at[slot, g, 1 - side],
                        device_id={axis: to[side]},
                        device_id_type=pl.DeviceIdType.MESH,
                    )
                )
        return made

    def keep_edges(slot, g, i, t, value, low, high):
        if t == 0:
            z_sent[slot, g, 0, i : i + 1, :] = value[0:1]
        if t == tiles - 1:
            z_sent[slot, g, 1, i : i + 1, :] = value[TILE - 1 :]
        k = t * per + i
        turned = pltpu.roll(value, k, 1) if k else value
        low = jnp.where(lane == k, turned, low)
        high = jnp.where(lane == (k - 1) % LANES, turned, high)
        return low, high

    def prepare(g, _):
        low = high = jnp.zeros((TILE, LANES), jnp.float32)
        for p in range(per // 2):
            q = g * (per // 2) + p
            sig_e, sig_o = shift_ref[2 * q], shift_ref[2 * q + 1]
            c_e = signed_ref[2 * q]
            for t in order:
                span = pl.ds(t * TILE, TILE)
                mob, base = mob_ref[span, :], base_ref[span, :]
                d_e, d_o = sig_e + base, sig_o + base
                scale = damping / (d_e * d_o + c_e * c_e)
                s_e, s_o = spec_ref[2 * q, span, :], spec_ref[2 * q + 1, span, :]
                b_e = scale * (d_o * s_e - c_e * s_o)
                b_o = scale * (d_e * s_o + c_e * s_e)
                scaled = scale * mob
                gain[2 * q, span, :] = scaled * d_o
                gain[2 * q + 1, span, :] = scaled * d_e
                cross[q, span, :] = scaled * c_e
                start_val[2 * q, span, :] = b_e
                start_val[2 * q + 1, span, :] = b_o
                own = pl.ds((t + 1) * TILE, TILE)
                state_a[2 * q, own, :] = b_e
                state_a[2 * q + 1, own, :] = b_o
                low, high = keep_edges(0, g, 2 * p, t, b_e, low, high)
                low, high = keep_edges(0, g, 2 * p + 1, t, b_o, low, high)
        c_sent[0, g, 0] = low
        c_sent[0, g, 1] = high
        for copy in copies(0, g):
            copy.start()
        return 0

    lax.fori_loop(0, groups, prepare, 0)

    def sweep(now, source, target, send):
        later = 1 - now

        def one_group(g, _):
            for copy in copies(now, g):
                copy.wait()
            from_left, from_right = c_halo[now, g, 0], c_halo[now, g, 1]
            low = high = jnp.zeros((TILE, LANES), jnp.float32)
            for i in range(per):
                m = g * per + i
                source[m, pl.ds(TILE - 1, 1), :] = z_halo[now, g, 0, i : i + 1, :]
                source[m, pl.ds(TILE + rows, 1), :] = z_halo[now, g, 1, i : i + 1, :]

            def around(m, i, t):
                top = (t + 1) * TILE
                mid = source[m, pl.ds(top, TILE), :]
                k = t * per + i
                edge = jnp.where(lane == k, from_right, from_left)
                edge = pltpu.roll(edge, LANES - k, 1) if k else edge
                total = source[m, pl.ds(top - 1, TILE), :] + source[m, pl.ds(top + 1, TILE), :]
                right = pltpu.roll(jnp.where(lane == 0, edge, mid), LANES - 1, 1)
                left = pltpu.roll(jnp.where(lane == LANES - 1, edge, mid), 1, 1)
                return mid, total + (left + right)

            for p in range(per // 2):
                q = g * (per // 2) + p
                news = []
                for t in range(tiles):
                    span = pl.ds(t * TILE, TILE)
                    y_e, n_e = around(2 * q, 2 * p, t)
                    y_o, n_o = around(2 * q + 1, 2 * p + 1, t)
                    c = cross[q, span, :]
                    new_e = keep * y_e + start_val[2 * q, span, :] + (gain[2 * q, span, :] * n_e - c * n_o)
                    new_o = keep * y_o + start_val[2 * q + 1, span, :] + (gain[2 * q + 1, span, :] * n_o + c * n_e)
                    news.append((new_e, new_o))
                for t, (new_e, new_o) in enumerate(news):
                    own = pl.ds((t + 1) * TILE, TILE)
                    target[2 * q, own, :] = new_e
                    target[2 * q + 1, own, :] = new_o
                    if send:
                        low, high = keep_edges(later, g, 2 * p, t, new_e, low, high)
                        low, high = keep_edges(later, g, 2 * p + 1, t, new_o, low, high)
            if send:
                c_sent[later, g, 0] = low
                c_sent[later, g, 1] = high
                for copy in copies(later, g):
                    copy.start()
            return 0

        lax.fori_loop(0, groups, one_group, 0)

    def two_sweeps(s, _):
        sweep(0, state_a, state_b, True)
        sweep(1, state_b, state_a, True)
        return 0

    count = SWEEPS - 1
    lax.fori_loop(0, (count - 1) // 2, two_sweeps, 0)
    if count % 2 == 0:
        sweep(0, state_a, state_b, True)
        sweep(1, state_b, state_a, False)
    else:
        sweep(0, state_a, state_b, False)
    last = state_b if count % 2 else state_a

    def store(m, _):
        out_ref[m] = last[m, TILE : TILE + rows, :]
        return 0

    lax.fori_loop(0, coefs, store, 0)


def fits_block(coefs, rows, cols):
    tiles = rows // TILE
    return (
        cols == LANES and rows % TILE == 0 and LANES % tiles == 0
        and (LANES // tiles) % 8 == 0 and coefs % (LANES // tiles) == 0
    )


def relax_block(spectrum, shifts, signed, frozen, mobility):
    coefs, rows, cols = spectrum.shape
    per = LANES // (rows // TILE)
    groups = coefs // per
    vmem = pl.BlockSpec(memory_space=pltpu.VMEM)
    smem = pl.BlockSpec(memory_space=pltpu.SMEM)
    sems = pltpu.SemaphoreType.DMA((2, groups, 2))
    return pl.pallas_call(
        functools.partial(block_kernel, lax.axis_size("space"), lax.axis_size("tm")),
        out_shape=jax.ShapeDtypeStruct(spectrum.shape, jnp.float32),
        in_specs=[smem, smem, vmem, vmem, vmem],
        out_specs=vmem,
        scratch_shapes=[
            pltpu.VMEM((coefs, rows + 2 * TILE, cols), jnp.float32),
            pltpu.VMEM((coefs, rows + 2 * TILE, cols), jnp.float32),
            pltpu.VMEM((coefs, rows, cols), jnp.float32),
            pltpu.VMEM((coefs // 2, rows, cols), jnp.float32),
            pltpu.VMEM((coefs, rows, cols), jnp.float32),
            pltpu.VMEM((2, groups, 2, per, cols), jnp.float32),
            pltpu.VMEM((2, groups, 2, per, cols), jnp.float32),
            pltpu.VMEM((2, groups, 2, TILE, LANES), jnp.float32),
            pltpu.VMEM((2, groups, 2, TILE, LANES), jnp.float32),
            sems, sems, sems, sems,
        ],
        compiler_params=pltpu.CompilerParams(
            collective_id=1, has_side_effects=True, vmem_limit_bytes=32 * 1024 * 1024
        ),
    )(shifts, signed, spectrum, frozen + 4.0 * mobility, mobility)


def precondition_columns(values, frozen, mobility, tables):
    forward, inverse, shifts, signed, weights = tables
    width = values.shape[2] // lax.axis_size("tm")
    first = lax.axis_index("tm") * width
    own_frozen = lax.dynamic_slice_in_dim(frozen, first, width, axis=1)
    own_mobility = lax.dynamic_slice_in_dim(mobility, first, width, axis=1)
    weighted = forward * weights[None, :]
    gathered = lax.all_to_all(values, "tm", split_axis=2, concat_axis=0, tiled=True)
    spectrum = jnp.einsum("mj,jrc->mrc", weighted, gathered, precision=lax.Precision.HIGHEST)
    solved = relax_block(spectrum, shifts, signed, own_frozen, own_mobility)
    restoring = inverse / weights[:, None]
    in_time = jnp.einsum("jm,mrc->jrc", restoring, solved, precision=lax.Precision.HIGHEST)
    return lax.all_to_all(in_time, "tm", split_axis=0, concat_axis=2, tiled=True)


def sum_kernel(t_count, z_count, x_ref, out_ref, t_got, z_own, z_got, t_send, t_recv, z_send, z_recv):
    barrier = pltpu.get_barrier_semaphore()
    places = (("tm", t_count), ("space", z_count))
    for axis, count in places:
        me = lax.axis_index(axis)
        for k in range(1, count):
            pl.semaphore_signal(
                barrier, inc=1, device_id={axis: lax.rem(me + k, count)},
                device_id_type=pl.DeviceIdType.MESH,
            )
    pl.semaphore_wait(barrier, t_count + z_count - 2)
    for axis, count, src, got, snd, rcv in (
        ("tm", t_count, x_ref, t_got, t_send, t_recv),
        ("space", z_count, z_own, z_got, z_send, z_recv),
    ):
        me = lax.axis_index(axis)
        made = []
        for k in range(1, count):
            made.append(
                pltpu.make_async_remote_copy(
                    src_ref=src, dst_ref=got.at[me], send_sem=snd.at[k], recv_sem=rcv.at[k],
                    device_id={axis: lax.rem(me + k, count)},
                    device_id_type=pl.DeviceIdType.MESH,
                )
            )
        for copy in made:
            copy.start()
        got[me] = src[...]
        for copy in made:
            copy.wait()
        total = got[0]
        for k in range(1, count):
            total = total + got[k]
        if axis == "tm":
            z_own[...] = total
        else:
            out_ref[...] = total


def summed(parts):
    t_count, z_count = lax.axis_size("tm"), lax.axis_size("space")
    row = lax.broadcasted_iota(jnp.int32, (TILE, LANES), 0)
    packed = jnp.zeros((TILE, LANES), jnp.float32)
    for k, part in enumerate(parts):
        packed = jnp.where(row == k, part, packed)
    vmem = pl.BlockSpec(memory_space=pltpu.VMEM)
    dma = pltpu.SemaphoreType.DMA
    total = pl.pallas_call(
        functools.partial(sum_kernel, t_count, z_count),
        out_shape=jax.ShapeDtypeStruct((TILE, LANES), jnp.float32),
        in_specs=[vmem],
        out_specs=vmem,
        scratch_shapes=[
            pltpu.VMEM((t_count, TILE, LANES), jnp.float32),
            pltpu.VMEM((TILE, LANES), jnp.float32),
            pltpu.VMEM((z_count, TILE, LANES), jnp.float32),
            dma((t_count,)), dma((t_count,)), dma((z_count,)), dma((z_count,)),
        ],
        compiler_params=pltpu.CompilerParams(
            collective_id=2, has_side_effects=True, vmem_limit_bytes=4 * 1024 * 1024
        ),
    )(packed)
    return [total[k, 0] for k in range(len(parts))]


def jacobian(values, trajectory, mobility):
    arriving = passed_along(values[-1:], "tm", 1)
    earlier = jnp.concatenate([arriving, values[:-1]], axis=0)
    reaction = reaction_scale * (3.0 * trajectory * trajectory - 1.0)
    return (values - earlier) / time_step + mobility[None] * neg_laplace(values) + reaction * values


def on_device(trajectory, initial_state, residual, mobility):
    tables = time_tables(NT)
    frozen = reaction_scale * jnp.maximum(3.0 * initial_state * initial_state - 1.0, 0.0)
    steps_dev, rows, cols = residual.shape
    shards = lax.axis_size("tm")
    by_columns = cols % shards == 0 and fits_block(NT, rows, cols // shards)
    run = precondition_columns if by_columns else precondition
    direction = run(residual, frozen, mobility, tables)
    applied = jacobian(direction, trajectory, mobility)
    norm_square, cross_sum, squared_applied = summed(
        (jnp.sum(residual * residual), jnp.sum(residual * applied), jnp.sum(applied * applied))
    )
    projection = cross_sum / norm_square
    squared_sum = squared_applied / norm_square
    remainder = jnp.maximum(squared_sum - projection * projection, 0.0)
    update = cross_sum / squared_applied * direction
    reduction = jnp.sqrt(remainder / squared_sum)
    return (update, reduction)


def solution(mesh):
    placed = (P("tm", "space", None), P("space", None), P("tm", "space", None), P("space", None))
    return jax.shard_map(
        on_device,
        mesh=mesh,
        in_specs=placed,
        out_specs=(P("tm", "space", None), P()),
        check_vma=False,
    )
```

```python
import functools
import jax
import jax.numpy as jnp
from jax import lax
from jax.experimental import pallas as pl
from jax.experimental.pallas import tpu as pltpu
from jax.sharding import PartitionSpec as P

NT = 64
SWEEPS = 16


circ_weight = 0.2
time_step = 0.01
damping = 0.8
reaction_scale = 40.0


def padded_2(block, sides, width):
    for axis, dim in sides:
        count = lax.axis_size(axis)
        forward = [(i, i + 1) for i in range(count - 1)]
        forward.append((count - 1, 0))
        backward = [(target, source) for source, target in forward]
        low = lax.ppermute(
            lax.slice_in_dim(block, block.shape[dim] - width, None, axis=dim), axis, forward
        )
        high = lax.ppermute(lax.slice_in_dim(block, 0, width, axis=dim), axis, backward)
        block = jnp.concatenate([low, block, high], axis=dim)
    return block


def passed_along(block, axis, distance):
    devices = range(lax.axis_size(axis))
    route = [(i - distance, i) for i in devices if i - distance in devices]
    return lax.ppermute(block, axis, route)


def time_tables(step_count):
    positions = jnp.arange(step_count).astype(jnp.float32)
    pair_ids = jnp.arange(step_count // 2).astype(jnp.float32)
    phases = 2.0 * jnp.pi * pair_ids / step_count
    angles = phases[:, None] * positions[None, :]
    forward = jnp.stack([jnp.cos(angles), -jnp.sin(angles)], axis=1).reshape(step_count, step_count)
    row_id = jnp.arange(step_count)[:, None]
    forward = jnp.where(row_id == 1, jnp.cos(jnp.pi * positions)[None, :], forward)
    scaling = jnp.where(jnp.arange(step_count) < 2, 1.0, 2.0) / step_count
    inverse = forward.T * scaling[None, :]
    factor = circ_weight ** (1.0 / step_count)
    shift_pair = (1.0 - factor * jnp.cos(phases)) / time_step
    shifts = jnp.stack([shift_pair, shift_pair], axis=1).reshape(step_count)
    shifts = shifts.at[1].set((1.0 + factor) / time_step)
    coupling = factor * jnp.sin(phases) / time_step
    signed = jnp.stack([-coupling, coupling], axis=1).reshape(step_count)
    weights = circ_weight ** (positions / step_count)
    return (forward, inverse, shifts, signed, weights)


def neg_laplace(values):
    padded = padded_2(values, (("space", 1),), 1)
    middle = padded[:, 1:-1, :]
    neighbours = padded[:, 2:, :] + padded[:, :-2, :]
    neighbours = neighbours + jnp.roll(middle, 1, axis=2) + jnp.roll(middle, -1, axis=2)
    return 4.0 * values - neighbours


TILE = 8


def relax_kernel(
    count, shift_ref, signed_ref, spec_ref, base_ref, mob_ref, out_ref,
    state, gain, cross, start_val, sent, halo, send_sem, recv_sem,
):
    coefs, rows, cols = spec_ref.shape
    pairs, tiles = coefs // 2, rows // TILE
    keep = 1.0 - damping
    me = lax.axis_index("space")
    prev, after = lax.rem(me + count - 1, count), lax.rem(me + 1, count)

    barrier = pltpu.get_barrier_semaphore()
    for other in (prev, after):
        pl.semaphore_signal(
            barrier, inc=1, device_id={"space": other}, device_id_type=pl.DeviceIdType.MESH
        )
    pl.semaphore_wait(barrier, 2)

    def edge(slot, q, side):
        return pltpu.make_async_remote_copy(
            src_ref=sent.at[slot, q, side],
            dst_ref=halo.at[slot, q, 1 - side],
            send_sem=send_sem.at[slot, q, side],
            recv_sem=recv_sem.at[slot, q, 1 - side],
            device_id={"space": prev if side == 0 else after},
            device_id_type=pl.DeviceIdType.MESH,
        )

    def send(slot, q):
        for side in range(2):
            edge(slot, q, side).start()

    def prepare(q, _):
        sig_e, sig_o = shift_ref[2 * q], shift_ref[2 * q + 1]
        c_e = signed_ref[2 * q]
        for t in [0, tiles - 1] + list(range(1, tiles - 1)):
            span = pl.ds(t * TILE, TILE)
            mob, base = mob_ref[span, :], base_ref[span, :]
            d_e, d_o = sig_e + base, sig_o + base
            scale = damping / (d_e * d_o + c_e * c_e)
            s_e, s_o = spec_ref[2 * q, span, :], spec_ref[2 * q + 1, span, :]
            b_e = scale * (d_o * s_e - c_e * s_o)
            b_o = scale * (d_e * s_o + c_e * s_e)
            scaled = scale * mob
            gain[2 * q, span, :] = scaled * d_o
            gain[2 * q + 1, span, :] = scaled * d_e
            cross[q, span, :] = scaled * c_e
            start_val[2 * q, span, :] = b_e
            start_val[2 * q + 1, span, :] = b_o
            own = pl.ds((t + 1) * TILE, TILE)
            state[0, 2 * q, own, :] = b_e
            state[0, 2 * q + 1, own, :] = b_o
            if t == 0:
                sent[0, q, 0, 0:1, :] = b_e[0:1]
                sent[0, q, 0, 1:2, :] = b_o[0:1]
            if t == tiles - 1:
                sent[0, q, 1, 0:1, :] = b_e[TILE - 1 :]
                sent[0, q, 1, 1:2, :] = b_o[TILE - 1 :]
                send(0, q)
        return 0

    lax.fori_loop(0, pairs, prepare, 0)

    def around(slot, m, t):
        top = (t + 1) * TILE
        mid = state[slot, m, pl.ds(top, TILE), :]
        total = state[slot, m, pl.ds(top - 1, TILE), :] + state[slot, m, pl.ds(top + 1, TILE), :]
        total = total + (pltpu.roll(mid, 1, 1) + pltpu.roll(mid, cols - 1, 1))
        return mid, total

    def sweep(s, _):
        now = lax.rem(s, 2)
        later = 1 - now

        def one_pair(q, _):
            for side in range(2):
                edge(now, q, side).wait()
            for part in range(2):
                state[now, 2 * q + part, pl.ds(TILE - 1, 1), :] = halo[now, q, 0, part : part + 1, :]
                state[now, 2 * q + part, pl.ds(TILE + rows, 1), :] = halo[now, q, 1, part : part + 1, :]
            for t in [0, tiles - 1] + list(range(1, tiles - 1)):
                span = pl.ds(t * TILE, TILE)
                own = pl.ds((t + 1) * TILE, TILE)
                y_e, n_e = around(now, 2 * q, t)
                y_o, n_o = around(now, 2 * q + 1, t)
                c = cross[q, span, :]
                new_e = keep * y_e + start_val[2 * q, span, :] + (gain[2 * q, span, :] * n_e - c * n_o)
                new_o = keep * y_o + start_val[2 * q + 1, span, :] + (gain[2 * q + 1, span, :] * n_o + c * n_e)
                state[later, 2 * q, own, :] = new_e
                state[later, 2 * q + 1, own, :] = new_o
                if t == 0:
                    sent[later, q, 0, 0:1, :] = new_e[0:1]
                    sent[later, q, 0, 1:2, :] = new_o[0:1]
                if t == tiles - 1:
                    sent[later, q, 1, 0:1, :] = new_e[TILE - 1 :]
                    sent[later, q, 1, 1:2, :] = new_o[TILE - 1 :]

                    @pl.when(s < SWEEPS - 2)
                    def _():
                        send(later, q)

            return 0

        return lax.fori_loop(0, pairs, one_pair, 0)

    lax.fori_loop(0, SWEEPS - 1, sweep, 0)
    last = (SWEEPS - 1) % 2

    def store(m, _):
        out_ref[m] = state[last, m, TILE : TILE + rows, :]
        return 0

    lax.fori_loop(0, coefs, store, 0)


def relax_pairs(spectrum, shifts, signed, frozen, mobility):
    coefs, rows, cols = spectrum.shape
    pairs = coefs // 2
    count = lax.axis_size("space")
    vmem = pl.BlockSpec(memory_space=pltpu.VMEM)
    smem = pl.BlockSpec(memory_space=pltpu.SMEM)
    return pl.pallas_call(
        functools.partial(relax_kernel, count),
        out_shape=jax.ShapeDtypeStruct(spectrum.shape, jnp.float32),
        in_specs=[smem, smem, vmem, vmem, vmem],
        out_specs=vmem,
        scratch_shapes=[
            pltpu.VMEM((2, coefs, rows + 2 * TILE, cols), jnp.float32),
            pltpu.VMEM((coefs, rows, cols), jnp.float32),
            pltpu.VMEM((pairs, rows, cols), jnp.float32),
            pltpu.VMEM((coefs, rows, cols), jnp.float32),
            pltpu.VMEM((2, pairs, 2, 2, cols), jnp.float32),
            pltpu.VMEM((2, pairs, 2, 2, cols), jnp.float32),
            pltpu.SemaphoreType.DMA((2, pairs, 2)),
            pltpu.SemaphoreType.DMA((2, pairs, 2)),
        ],
        compiler_params=pltpu.CompilerParams(
            collective_id=0, has_side_effects=True, vmem_limit_bytes=32 * 1024 * 1024
        ),
    )(shifts, signed, spectrum, frozen + 4.0 * mobility, mobility)


def precondition(values, frozen, mobility, tables):
    forward, inverse, shifts, signed, weights = tables
    steps_dev = values.shape[0]
    time_rank = lax.axis_index("tm")
    offset = time_rank * steps_dev
    own_weights = lax.dynamic_slice_in_dim(weights, offset, steps_dev)
    own_shifts = lax.dynamic_slice_in_dim(shifts, offset, steps_dev)
    own_signed = lax.dynamic_slice_in_dim(signed, offset, steps_dev)
    weighted = own_weights[:, None, None] * values
    spectrum = jnp.einsum(
        "mj,jrc->mrc",
        forward,
        lax.all_to_all(weighted, "tm", split_axis=1, concat_axis=0, tiled=True),
        precision=lax.Precision.HIGHEST,
    )
    owned_part = lax.all_to_all(spectrum, "tm", split_axis=0, concat_axis=1, tiled=True)
    solved = relax_pairs(owned_part, own_shifts, own_signed, frozen, mobility)
    in_time = jnp.einsum(
        "jm,mrc->jrc",
        inverse,
        lax.all_to_all(solved, "tm", split_axis=1, concat_axis=0, tiled=True),
        precision=lax.Precision.HIGHEST,
    )
    restored = lax.all_to_all(in_time, "tm", split_axis=0, concat_axis=1, tiled=True)
    return restored / own_weights[:, None, None]


LANES = 128


def sum_kernel(t_count, z_count, x_ref, out_ref, t_got, z_own, z_got, t_send, t_recv, z_send, z_recv):
    barrier = pltpu.get_barrier_semaphore()
    places = (("tm", t_count), ("space", z_count))
    for axis, count in places:
        me = lax.axis_index(axis)
        for k in range(1, count):
            pl.semaphore_signal(
                barrier, inc=1, device_id={axis: lax.rem(me + k, count)},
                device_id_type=pl.DeviceIdType.MESH,
            )
    pl.semaphore_wait(barrier, t_count + z_count - 2)
    for axis, count, src, got, snd, rcv in (
        ("tm", t_count, x_ref, t_got, t_send, t_recv),
        ("space", z_count, z_own, z_got, z_send, z_recv),
    ):
        me = lax.axis_index(axis)
        made = []
        for k in range(1, count):
            made.append(
                pltpu.make_async_remote_copy(
                    src_ref=src, dst_ref=got.at[me], send_sem=snd.at[k], recv_sem=rcv.at[k],
                    device_id={axis: lax.rem(me + k, count)},
                    device_id_type=pl.DeviceIdType.MESH,
                )
            )
        for copy in made:
            copy.start()
        got[me] = src[...]
        for copy in made:
            copy.wait()
        total = got[0]
        for k in range(1, count):
            total = total + got[k]
        if axis == "tm":
            z_own[...] = total
        else:
            out_ref[...] = total


def summed(parts):
    t_count, z_count = lax.axis_size("tm"), lax.axis_size("space")
    row = lax.broadcasted_iota(jnp.int32, (TILE, LANES), 0)
    packed = jnp.zeros((TILE, LANES), jnp.float32)
    for k, part in enumerate(parts):
        packed = jnp.where(row == k, part, packed)
    vmem = pl.BlockSpec(memory_space=pltpu.VMEM)
    dma = pltpu.SemaphoreType.DMA
    total = pl.pallas_call(
        functools.partial(sum_kernel, t_count, z_count),
        out_shape=jax.ShapeDtypeStruct((TILE, LANES), jnp.float32),
        in_specs=[vmem],
        out_specs=vmem,
        scratch_shapes=[
            pltpu.VMEM((t_count, TILE, LANES), jnp.float32),
            pltpu.VMEM((TILE, LANES), jnp.float32),
            pltpu.VMEM((z_count, TILE, LANES), jnp.float32),
            dma((t_count,)), dma((t_count,)), dma((z_count,)), dma((z_count,)),
        ],
        compiler_params=pltpu.CompilerParams(
            collective_id=2, has_side_effects=True, vmem_limit_bytes=4 * 1024 * 1024
        ),
    )(packed)
    return [total[k, 0] for k in range(len(parts))]


def jacobian(values, trajectory, mobility):
    arriving = passed_along(values[-1:], "tm", 1)
    earlier = jnp.concatenate([arriving, values[:-1]], axis=0)
    reaction = reaction_scale * (3.0 * trajectory * trajectory - 1.0)
    return (values - earlier) / time_step + mobility[None] * neg_laplace(values) + reaction * values


def on_device(trajectory, initial_state, residual, mobility):
    tables = time_tables(NT)
    frozen = reaction_scale * jnp.maximum(3.0 * initial_state * initial_state - 1.0, 0.0)
    direction = precondition(residual, frozen, mobility, tables)
    applied = jacobian(direction, trajectory, mobility)
    norm_square, cross_sum, squared_applied = summed(
        (jnp.sum(residual * residual), jnp.sum(residual * applied), jnp.sum(applied * applied))
    )
    projection = cross_sum / norm_square
    squared_sum = squared_applied / norm_square
    remainder = jnp.maximum(squared_sum - projection * projection, 0.0)
    update = cross_sum / squared_applied * direction
    reduction = jnp.sqrt(remainder / squared_sum)
    return (update, reduction)


def solution(mesh):
    placed = (P("tm", "space", None), P("space", None), P("tm", "space", None), P("space", None))
    return jax.shard_map(
        on_device,
        mesh=mesh,
        in_specs=placed,
        out_specs=(P("tm", "space", None), P()),
        check_vma=False,
    )
```
